512 devices in a mesh: row: 16 (over x, y_lo), col: 32 (over z, y_hi, core).
Axes of the slice: x: 4, y: 8 (y_hi: 2, y_lo: 4; y = y_hi * 4 + y_lo), z: 8, core: 2. Of those that a mesh axis runs over, the one named last changes fastest.
Arguments:
- object_field: float32 [2, 4096, 8192], P(None, 'row', 'col'), may hold values from -5 to 5
- velocity: float32 [2, 4096, 8192], P(None, 'row', 'col'), may hold values from -5 to 5
- positions: int32 [16, 32, 1, 2], P('row', 'col'), may hold values from 0 to 128
- measured: float32 [16, 32, 1, 256, 256], P('row', 'col'), may hold values from 0 to 2
- probe: float32 [2, 256, 256], replicated, may hold values from -5 to 5
Outputs:
- object_out: float32 [2, 4096, 8192], P(None, 'row', 'col')
- velocity_out: float32 [2, 4096, 8192], P(None, 'row', 'col')
The draws below stay inside these ranges and needn't reach their ends.
All inputs are finite; a program needn't handle non-finite values.
Results may differ from the reference program's by a relative error of at most 0.00018.
Values sent between devices are 32-bit elements; how exact they have to be, the bound alone decides.
A program may use at most 64 MiB of HBM per device.

```python
import math
import jax
import jax.numpy as jnp
from jax import lax

TILE = 256
P_SIZE = 256
W = 128
POS = 1
ITERS = 2
TILES_R = 16
TILES_C = 32
NY = 4096
NX = 8192
N_ROW = 16
N_COL = 32


def set_ends(array, rng, low, largest):
    dims = array.shape
    index_at = [jax.random.randint(jax.random.fold_in(rng, axis), (), 0, dims[axis]) for axis in range(len(dims))]
    array = array.at[tuple(index_at)].set(low)
    longest = dims.index(max(dims))
    index_at[longest] = (index_at[longest] + 1) % dims[longest]
    return array.at[tuple(index_at)].set(largest)


def shard_levels(key, dims, shards, low, largest):
    def one(position, shards_of):
        draws = jax.random.uniform(jax.random.fold_in(jax.random.fold_in(key, 6), position), (shards_of,), jnp.float32, low / len(shards), largest / len(shards))
        return jnp.repeat(jnp.exp(draws), dims[position] // shards_of).reshape((-1,) + (1,) * (len(dims) - position - 1))

    factor_of = one(*shards[0])
    for cut in shards[1:]:
        factor_of = factor_of * one(*cut)
    return factor_of


def normal_values(own_key, extent, deviation, most, shards=(), held_as=jnp.bfloat16):
    entries = jax.random.normal(own_key, extent, jnp.float32) * deviation
    if len(shards) > 0:
        entries = shard_levels(own_key, extent, shards, -0.22, 0.18) * entries
    return jnp.clip(entries, min=-most, max=most).astype(held_as)


def setup_inputs(seed: int = 0) -> dict:
    keys = jax.random.split(jax.random.key(seed), 6)
    object_field = normal_values(keys[0], (2, NY, NX), 0.7, 5.0, ((1, 16), (2, 32)), jnp.float32)
    velocity = normal_values(keys[1], (2, NY, NX), 0.5, 5.0, ((1, 16), (2, 32)), jnp.float32)
    positions = set_ends(jax.random.randint(keys[2], (TILES_R, TILES_C, POS, 2), 0, TILE + W - P_SIZE + 1), jax.random.fold_in(keys[2], 1), 0, TILE + W - P_SIZE).astype(jnp.int32)
    measured = jnp.clip(2.0 * jax.random.uniform(keys[3], (TILES_R, TILES_C, POS, P_SIZE, P_SIZE), jnp.float32) ** shard_levels(keys[3], (TILES_R, TILES_C, POS, P_SIZE, P_SIZE), ((0, 16), (1, 32)), -0.2, 0.2), 0.0, 2.0)
    probe = normal_values(keys[4], (2, P_SIZE, P_SIZE), 0.7, 5.0, (), jnp.float32)
    return {"object_field": object_field, "velocity": velocity, "positions": positions, "measured": measured, "probe": probe}


step_size = 0.1
momentum_rate = 0.8

def fourier_tables(length):
    index = jnp.arange(length, dtype=jnp.int32)
    phase = index[:, None] * index[None, :] % length
    angle = -2.0 * math.pi * phase.astype(jnp.float32) / length
    scale = 1.0 / math.sqrt(length)
    return (jnp.cos(angle) * scale, jnp.sin(angle) * scale)

def left_product(table_re, table_im, field_re, field_im):
    hp = lax.Precision.HIGHEST

    def mult(a, b):
        return jnp.einsum('jk,pkl->pjl', a, b, precision=hp)
    return (mult(table_re, field_re) - mult(table_im, field_im), mult(table_re, field_im) + mult(table_im, field_re))

def right_product(field_re, field_im, table_re, table_im):
    hp = lax.Precision.HIGHEST

    def mult(a, b):
        return jnp.einsum('pjk,kl->pjl', a, b, precision=hp)
    return (mult(field_re, table_re) - mult(field_im, table_im), mult(field_re, table_im) + mult(field_im, table_re))

def patch_gradients(patches, intensity, probe, table_re, table_im):
    probe_re = probe[0][None]
    probe_im = probe[1][None]
    exit_re = probe_re * patches[0] - probe_im * patches[1]
    exit_im = probe_re * patches[1] + probe_im * patches[0]
    far_re, far_im = left_product(table_re, table_im, exit_re, exit_im)
    far_re, far_im = right_product(far_re, far_im, table_re, table_im)
    misfit = far_re * far_re + far_im * far_im - intensity
    back_re, back_im = (misfit * far_re, misfit * far_im)
    back_re, back_im = left_product(table_re, -table_im, back_re, back_im)
    back_re, back_im = right_product(back_re, back_im, table_re, -table_im)
    out_re = probe_re * back_re + probe_im * back_im
    out_im = probe_re * back_im - probe_im * back_re
    return jnp.stack([out_re, out_im])

def reference(object_field, velocity, positions, measured, probe):
    table_re, table_im = fourier_tables(P_SIZE)
    count = N_ROW * N_COL * POS
    for sweep in range(ITERS):
        extended = jnp.pad(object_field, ((0, 0), (0, W), (0, W)))

        def add_window(number, gradient):
            number = number.astype(jnp.int32)
            tile_row = number // (N_COL * POS)
            tile_col = number // POS % N_COL
            which = number % POS
            top = (tile_row * TILE + positions[tile_row, tile_col, which, 0]).astype(jnp.int32)
            leftmost = (tile_col * TILE + positions[tile_row, tile_col, which, 1]).astype(jnp.int32)
            zero = jnp.zeros((), jnp.int32)
            patch = lax.dynamic_slice(extended, (zero, top, leftmost), (2, P_SIZE, P_SIZE))
            intensity = measured[tile_row, tile_col, which][None]
            piece = patch_gradients(patch[:, None], intensity, probe, table_re, table_im)[:, 0]
            current = lax.dynamic_slice(gradient, (zero, top, leftmost), (2, P_SIZE, P_SIZE))
            return lax.dynamic_update_slice(gradient, current + piece, (zero, top, leftmost))
        gradient = lax.fori_loop(0, count, add_window, jnp.zeros_like(extended))
        gradient = gradient[:, :NY, :NX]
        velocity = momentum_rate * velocity + gradient
        object_field = object_field - step_size * velocity
    return (object_field, velocity)
```

```python
import functools

import numpy as np

import jax
import jax.numpy as jnp
from jax import lax
from jax.experimental import pallas as pl
from jax.experimental.pallas import tpu as pltpu
from jax.sharding import PartitionSpec as P

N = 256
W = 128
ITERS = 2
STEP = 0.1
MOMENTUM = 0.8
MESH = pl.DeviceIdType.MESH
F32 = jnp.float32
BF16 = jnp.bfloat16

V_LEFT, V_RIGHT, H_BOTTOM, H_TOP = range(4)
TOP, BOTTOM = pl.ds(0, W), pl.ds(W, W)
LEFT, RIGHT = pl.ds(0, W), pl.ds(W, W)


def fourier_tables():
    index = np.arange(N)
    angle = -2.0 * np.pi * (index[:, None] * index[None, :] % N) / N
    parts = []
    for table in (np.cos(angle) / np.sqrt(N), np.sin(angle) / np.sqrt(N)):
        high = table.astype(BF16)
        parts += [high, (table - high.astype(np.float64)).astype(BF16)]
    return np.stack(parts)


def split(value):
    high = value.astype(BF16)
    return high, (value - high.astype(F32)).astype(BF16)


def kernel(
    n_rows, n_cols,
    pos_ref, obj_hbm, vel_hbm, meas_hbm, probe_hbm, table_hbm,
    obj_out, vel_out,
    obj, vel, obj1, vel1, meas, probe, table, right_table, left_table,
    stack, stack2, grad, recv, send, place, place_in,
    load_sem, store_sem, send_sem, recv_sem, place_send, place_recv,
):
    r = lax.axis_index("row")
    c = lax.axis_index("col")
    has = {
        (-1, 0): r > 0, (1, 0): r < n_rows - 1,
        (0, -1): c > 0, (0, 1): c < n_cols - 1,
    }

    loads = [
        pltpu.make_async_copy(src, dst, load_sem.at[i])
        for i, (src, dst) in enumerate(
            [(obj_hbm, obj), (table_hbm, table), (probe_hbm, probe), (meas_hbm, meas), (vel_hbm, vel)]
        )
    ]
    for load in loads:
        load.start()

    barrier = pltpu.get_barrier_semaphore()
    for (dr, dc), there in has.items():
        @pl.when(there)
        def _():
            pl.semaphore_signal(barrier, inc=1, device_id=(r + dr, c + dc), device_id_type=MESH)

    dy = pos_ref[0]
    dx = pos_ref[1]
    rows = lax.broadcasted_iota(jnp.int32, (W, W), 0)
    cols = lax.broadcasted_iota(jnp.int32, (W, W), 1)
    below = rows < dy
    beside = cols < dx
    rows_f = rows.astype(F32)
    cols_f = cols.astype(F32)
    place[...] = jnp.where(
        lax.broadcasted_iota(jnp.int32, (8, W), 0) == 0, dy.astype(F32), dx.astype(F32)
    )

    zeros = jnp.zeros((2, W, W), F32)
    for step in range(2 * ITERS):
        pull = step % 2 == 0
        edge_v = r == n_rows - 1 if pull else r == 0
        edge_h = c == n_cols - 1 if pull else c == 0

        @pl.when(edge_v)
        def _():
            recv[step * 4 + V_LEFT] = zeros
            recv[step * 4 + V_RIGHT] = zeros

        @pl.when(edge_h)
        def _():
            recv[step * 4 + H_BOTTOM] = zeros
            recv[step * 4 + H_TOP] = zeros

    @pl.when(c == 0)
    def _():
        place_in[0] = jnp.zeros((8, W), F32)

    @pl.when(r == 0)
    def _():
        place_in[1] = jnp.zeros((8, W), F32)

    pl.semaphore_wait(barrier, sum(there.astype(jnp.int32) for there in has.values()))

    def way(step, kind):
        d = -1 if step % 2 == 0 else 1
        return (d, 0) if kind in (V_LEFT, V_RIGHT) else (0, d)

    started = []

    def put(step, kind, src):
        dr, dc = way(step, kind)
        i = step * 4 + kind
        copy = pltpu.make_async_remote_copy(
            src_ref=src, dst_ref=recv.at[i], send_sem=send_sem.at[i], recv_sem=recv_sem.at[i],
            device_id=(r + dr, c + dc), device_id_type=MESH,
        )

        @pl.when(has[dr, dc])
        def _():
            copy.start()

        started.append((has[dr, dc], copy))

    def got(step, kind):
        dr, dc = way(step, kind)
        i = step * 4 + kind

        @pl.when(has[-dr, -dc])
        def _():
            pltpu.make_async_remote_copy(
                src_ref=recv.at[i], dst_ref=recv.at[i], send_sem=send_sem.at[i],
                recv_sem=recv_sem.at[i], device_id=(r + dr, c + dc), device_id_type=MESH,
            ).wait_recv()

        return recv[i]

    places = [
        ((0, 1), pltpu.make_async_remote_copy(
            src_ref=place, dst_ref=place_in.at[0], send_sem=place_send.at[0],
            recv_sem=place_recv.at[0], device_id=(r, c + 1), device_id_type=MESH)),
        ((1, 0), pltpu.make_async_remote_copy(
            src_ref=place, dst_ref=place_in.at[1], send_sem=place_send.at[1],
            recv_sem=place_recv.at[1], device_id=(r + 1, c), device_id_type=MESH)),
    ]

    def share_places():
        for to, copy in places:
            @pl.when(has[to])
            def _():
                copy.start()

    def pull_top(step, source, dy_left):
        low = got(step, V_LEFT)

        @pl.when(has[0, -1])
        def _():
            send[step * 4 + H_TOP] = jnp.where(
                rows_f < dy_left, low, source[:, TOP, LEFT]
            )

        put(step, H_TOP, send.at[step * 4 + H_TOP])

    loads[0].wait()
    share_places()
    put(0, V_LEFT, obj.at[:, TOP, LEFT])
    put(0, H_BOTTOM, obj.at[:, BOTTOM, LEFT])
    put(0, V_RIGHT, obj.at[:, TOP, RIGHT])

    loads[1].wait()
    re_high, re_low, im_high, im_low = (table[i] for i in range(4))
    blocks = [
        (re_high, im_high), (re_high, im_high), (re_low, im_low),
        (-im_high, re_high), (-im_high, re_high), (-im_low, re_low),
    ]
    for b, (real, imag) in enumerate(blocks):
        span = pl.ds(b * N, N)
        right_table[span, pl.ds(0, N)] = real
        right_table[span, pl.ds(N, N)] = imag
        for half in range(2):
            left_table[pl.ds(half * N, W), span] = real[half * W : (half + 1) * W]
            left_table[pl.ds(half * N + W, W), span] = imag[half * W : (half + 1) * W]

    loads[2].wait()
    for part in range(2):
        turned = pltpu.roll(probe[part], dy, 0)
        probe[part] = pltpu.roll(turned, dx, 1)

    for k, to in ((0, (0, -1)), (1, (-1, 0))):
        @pl.when(has[to])
        def _():
            places[k][1].wait_recv()

    dy_left = place_in[0, 0:1, :]
    dx_above = place_in[1, 1:2, :]
    beside_above = cols_f < dx_above
    pull_top(0, obj, dy_left)

    def put_stack(where, span_rows, span_cols, real, imag):
        for base, value in ((0, real), (3, imag)):
            high, low = split(value)
            for b, item in ((0, high), (1, low), (2, high)):
                where[span_rows, pl.ds((base + b) * N + span_cols, item.shape[1])] = item

    def put_stack2(row, real, imag):
        for base, value in ((0, real), (3, imag)):
            high, low = split(value)
            for b, item in ((0, high), (1, low), (2, high)):
                stack2[pl.ds((base + b) * N + row, item.shape[0]), :] = item

    def exit_wave(half, quarter_left, quarter_right):
        span = TOP if half == 0 else BOTTOM
        for side, patch in ((0, quarter_left), (1, quarter_right)):
            lanes = pl.ds(side * W, W)
            pr, pi = probe[0, span, lanes], probe[1, span, lanes]
            put_stack(
                stack, span, side * W,
                pr * patch[0] - pi * patch[1], pr * patch[1] + pi * patch[0],
            )

    def right_product(half):
        span = pl.ds(half * W, W)
        out = jnp.dot(stack[span, :], right_table[...], preferred_element_type=F32)
        put_stack2(half * W, out[:, :N], out[:, N:])

    def left_product(half):
        out = jnp.dot(
            left_table[pl.ds(half * N, N), :], stack2[...], preferred_element_type=F32
        )
        return out[:W], out[W:]

    def sweep(step, source):
        bottom = jnp.where(beside, got(step, H_BOTTOM), source[:, BOTTOM, LEFT])
        exit_wave(1, bottom, source[:, BOTTOM, RIGHT])
        right_product(1)
        top_right = jnp.where(below, got(step, V_RIGHT), source[:, TOP, RIGHT])
        own = jnp.where(below, recv[step * 4 + V_LEFT], source[:, TOP, LEFT])
        top_left = jnp.where(beside, got(step, H_TOP), own)
        exit_wave(0, top_left, top_right)
        right_product(0)
        for half in range(2):
            far_re, far_im = left_product(half)
            misfit = far_re * far_re + far_im * far_im - meas[pl.ds(half * W, W), :]
            put_stack(stack, pl.ds(half * W, W), 0, misfit * far_re, -(misfit * far_im))
        for half in range(2):
            right_product(half)
        push = step + 1
        for half in range(2):
            span = pl.ds(half * W, W)
            back_re, back_im = left_product(half)
            pr, pi = probe[0, span, :], probe[1, span, :]
            grad[0, span, :] = pr * back_re - pi * back_im
            grad[1, span, :] = -(pr * back_im) - pi * back_re
            if half == 0:
                for kind, lanes in ((V_LEFT, LEFT), (V_RIGHT, RIGHT)):
                    send[push * 4 + kind] = jnp.where(below, grad[:, TOP, lanes], 0.0)
                    put(push, kind, send.at[push * 4 + kind])
            else:
                send[push * 4 + H_BOTTOM] = jnp.where(beside, grad[:, BOTTOM, LEFT], 0.0)
                put(push, H_BOTTOM, send.at[push * 4 + H_BOTTOM])
        above = got(push, V_LEFT)
        send[push * 4 + H_TOP] = jnp.where(
            beside & ~below, grad[:, TOP, LEFT], 0.0
        ) + jnp.where(beside_above, above, 0.0)
        put(push, H_TOP, send.at[push * 4 + H_TOP])

    stores = []

    def update(last, old_obj, old_vel, new_obj, new_vel, span_r, span_c, gradient):
        speed = MOMENTUM * old_vel[:, span_r, span_c] + gradient
        new_vel[:, span_r, span_c] = speed
        new_obj[:, span_r, span_c] = old_obj[:, span_r, span_c] - STEP * speed
        if last:
            for src, dst in ((new_obj, obj_out), (new_vel, vel_out)):
                copy = pltpu.make_async_copy(
                    src.at[:, span_r, span_c], dst.at[:, span_r, span_c], store_sem.at[len(stores)]
                )
                copy.start()
                stores.append(copy)

    def settle(step, last, old_obj, old_vel, new_obj, new_vel):
        push, pull = step + 1, step + 2
        refs = (last, old_obj, old_vel, new_obj, new_vel)
        update(*refs, BOTTOM, RIGHT, grad[:, BOTTOM, RIGHT])
        gradient = jnp.where(below, 0.0, grad[:, TOP, RIGHT]) + got(push, V_RIGHT)
        update(*refs, TOP, RIGHT, gradient)
        if not last:
            put(pull, V_RIGHT, new_obj.at[:, TOP, RIGHT])
        gradient = jnp.where(beside, 0.0, grad[:, BOTTOM, LEFT]) + got(push, H_BOTTOM)
        update(*refs, BOTTOM, LEFT, gradient)
        if not last:
            put(pull, H_BOTTOM, new_obj.at[:, BOTTOM, LEFT])
        above = jnp.where(beside_above, 0.0, recv[push * 4 + V_LEFT])
        gradient = (
            jnp.where(below | beside, 0.0, grad[:, TOP, LEFT]) + above + got(push, H_TOP)
        )
        update(*refs, TOP, LEFT, gradient)
        if not last:
            put(pull, V_LEFT, new_obj.at[:, TOP, LEFT])
            pull_top(pull, new_obj, dy_left)

    loads[3].wait()
    sweep(0, obj)
    loads[4].wait()
    settle(0, False, obj, vel, obj1, vel1)
    sweep(2, obj1)
    first, rest = started[:4], started[4:]
    for there, copy in first:
        @pl.when(there)
        def _():
            copy.wait_send()

    settle(2, True, obj1, vel1, obj, vel)

    for there, copy in rest + [(has[to], copy) for to, copy in places]:
        @pl.when(there)
        def _():
            copy.wait_send()

    for copy in stores:
        copy.wait()


def on_device(n_rows, n_cols, object_field, velocity, positions, measured, probe):
    vmem = lambda *shape: pltpu.VMEM(shape, F32)
    anywhere = pl.BlockSpec(memory_space=pl.ANY)
    messages = 8 * ITERS
    field = jax.ShapeDtypeStruct((2, N, N), F32)
    return pl.pallas_call(
        functools.partial(kernel, n_rows, n_cols),
        out_shape=(field, field),
        in_specs=[pl.BlockSpec(memory_space=pltpu.SMEM)] + [anywhere] * 5,
        out_specs=(anywhere, anywhere),
        scratch_shapes=[
            vmem(2, N, N), vmem(2, N, N), vmem(2, N, N), vmem(2, N, N),
            vmem(N, N), vmem(2, N, N),
            pltpu.VMEM((4, N, N), BF16),
            pltpu.VMEM((6 * N, 2 * N), BF16),
            pltpu.VMEM((2 * N, 6 * N), BF16),
            pltpu.VMEM((N, 6 * N), BF16),
            pltpu.VMEM((6 * N, N), BF16),
            vmem(2, N, N),
            vmem(messages, 2, W, W), vmem(messages, 2, W, W),
            vmem(8, W), vmem(2, 8, W),
            pltpu.SemaphoreType.DMA((5,)), pltpu.SemaphoreType.DMA((8,)),
            pltpu.SemaphoreType.DMA((messages,)), pltpu.SemaphoreType.DMA((messages,)),
            pltpu.SemaphoreType.DMA((2,)), pltpu.SemaphoreType.DMA((2,)),
        ],
        compiler_params=pltpu.CompilerParams(collective_id=0, has_side_effects=True),
        name="ptycho",
    )(
        positions.reshape(2), object_field, velocity, measured.reshape(N, N), probe,
        jnp.asarray(fourier_tables()),
    )


def solution(mesh):
    placed = (
        P(None, "row", "col"),
        P(None, "row", "col"),
        P("row", "col", None, None),
        P("row", "col", None, None, None),
        P(),
    )
    return jax.shard_map(
        functools.partial(on_device, mesh.shape["row"], mesh.shape["col"]),
        mesh=mesh,
        in_specs=placed,
        out_specs=(P(None, "row", "col"), P(None, "row", "col")),
        check_vma=False,
    )
```

```python
import functools

import numpy as np

import jax
import jax.numpy as jnp
from jax import lax
from jax.experimental import pallas as pl
from jax.experimental.pallas import tpu as pltpu
from jax.sharding import PartitionSpec as P

N = 256
W = 128
ITERS = 2
STEP = 0.1
MOMENTUM = 0.8
MESH = pl.DeviceIdType.MESH
F32 = jnp.float32
BF16 = jnp.bfloat16

UP, DOWN, TO_LEFT, TO_RIGHT = (-1, 0), (1, 0), (0, -1), (0, 1)
MESSAGES = {
    "obj_ht": TO_LEFT, "obj_hb": TO_LEFT, "obj_vr": UP, "obj_vl": UP,
    "grad_vl": DOWN, "grad_vr": DOWN, "grad_hb": TO_RIGHT, "grad_ht": TO_RIGHT,
    "next_vr": UP, "next_hb": TO_LEFT, "next_ht": TO_LEFT, "next_vl": UP,
    "last_vl": DOWN, "last_vr": DOWN, "last_hb": TO_RIGHT, "last_ht": TO_RIGHT,
}
SLOT = {name: i for i, name in enumerate(MESSAGES)}
TOP, BOTTOM = pl.ds(0, W), pl.ds(W, W)
LEFT, RIGHT = pl.ds(0, W), pl.ds(W, W)


CFG = dict(R1pre="tr", R1post="b", mid="|bB", mid2="hHrR", R4pre="|r", R4post="b", sweep="bt")


def fourier_tables():
    index = np.arange(N)
    angle = -2.0 * np.pi * (index[:, None] * index[None, :] % N) / N
    parts = []
    for table in (np.cos(angle) / np.sqrt(N), np.sin(angle) / np.sqrt(N)):
        high = table.astype(BF16)
        parts += [high, (table - high.astype(np.float64)).astype(BF16)]
    return np.stack(parts)


def split(value):
    high = value.astype(BF16)
    return high, (value - high.astype(F32)).astype(BF16)


def kernel(
    n_rows, n_cols,
    pos_hbm, obj_hbm, vel_hbm, meas_hbm, probe_hbm, table_hbm,
    obj_out, vel_out,
    pos, obj, vel, obj1, vel1, meas, probe, table, right_table, left_table,
    stack, stack2, grad, halo, recv, send, place, place_in,
    load_sem, store_sem, send_sem, recv_sem, place_send, place_recv,
):
    r = lax.axis_index("row")
    c = lax.axis_index("col")
    has = {UP: r > 0, DOWN: r < n_rows - 1, TO_LEFT: c > 0, TO_RIGHT: c < n_cols - 1}

    barrier = pltpu.get_barrier_semaphore()
    for (dr, dc), there in has.items():
        @pl.when(there)
        def _():
            pl.semaphore_signal(barrier, inc=1, device_id=(r + dr, c + dc), device_id_type=MESH)

    loads = [
        pltpu.make_async_copy(src, dst, load_sem.at[i])
        for i, (src, dst) in enumerate([
            (pos_hbm, pos), (obj_hbm, obj), (table_hbm, table), (probe_hbm, probe),
            (meas_hbm, meas), (vel_hbm, vel),
        ])
    ]
    for load in loads:
        load.start()

    zeros = jnp.zeros((2, W, W), F32)
    for way in (UP, DOWN, TO_LEFT, TO_RIGHT):
        @pl.when(~has[-way[0], -way[1]])
        def _():
            for name, to in MESSAGES.items():
                if to == way:
                    recv[SLOT[name]] = zeros

    @pl.when(~has[UP])
    def _():
        place_in[...] = jnp.zeros((8, W), F32)

    loads[0].wait()
    dy = pos[0]
    dx = pos[1]
    rows = lax.broadcasted_iota(jnp.int32, (W, W), 0)
    cols = lax.broadcasted_iota(jnp.int32, (W, W), 1)
    below = rows < dy
    beside = cols < dx
    place[...] = jnp.full((8, W), dx.astype(F32))

    with jax.named_scope("wait_barrier"):
        pl.semaphore_wait(barrier, sum(there.astype(jnp.int32) for there in has.values()))

    started = {}

    def message(name, src):
        dr, dc = MESSAGES[name]
        i = SLOT[name]
        return pltpu.make_async_remote_copy(
            src_ref=src, dst_ref=recv.at[i], send_sem=send_sem.at[i], recv_sem=recv_sem.at[i],
            device_id=(r + dr, c + dc), device_id_type=MESH,
        )

    def put(name, src=None):
        copy = message(name, send.at[SLOT[name]] if src is None else src)
        there = has[MESSAGES[name]]

        @pl.when(there)
        def _():
            copy.start()

        started[name] = there, copy

    def got(name):
        dr, dc = MESSAGES[name]
        with jax.named_scope("wait_" + name):
            @pl.when(has[-dr, -dc])
            def _():
                message(name, recv.at[SLOT[name]]).wait_recv()

        return recv[SLOT[name]]

    def fill(name, value):
        send[SLOT[name]] = value

    place_copy = pltpu.make_async_remote_copy(
        src_ref=place, dst_ref=place_in, send_sem=place_send, recv_sem=place_recv,
        device_id=(r + 1, c), device_id_type=MESH,
    )
    with jax.named_scope("wait_load"):
        loads[1].wait()

    @pl.when(has[DOWN])
    def _():
        place_copy.start()

    first = {
        "t": ("obj_ht", obj.at[:, TOP, LEFT]),
        "b": ("obj_hb", obj.at[:, BOTTOM, LEFT]),
        "r": ("obj_vr", obj.at[:, TOP, RIGHT]),
    }
    for k in CFG["R1pre"]:
        put(*first[k])

    def build_tables():
        re_high, re_low, im_high, im_low = (table[i] for i in range(4))
        blocks = [
            (re_high, im_high), (re_high, im_high), (re_low, im_low),
            (-im_high, re_high), (-im_high, re_high), (-im_low, re_low),
        ]
        for b, (real, imag) in enumerate(blocks):
            span = pl.ds(b * N, N)
            right_table[span, pl.ds(0, N)] = real
            right_table[span, pl.ds(N, N)] = imag
            for half in range(2):
                left_table[pl.ds(half * N, W), span] = real[half * W : (half + 1) * W]
                left_table[pl.ds(half * N + W, W), span] = imag[half * W : (half + 1) * W]

    def turn_probe():
        for part in range(2):
            turned = pltpu.roll(probe[part], dy, 0)
            probe[part] = pltpu.roll(turned, dx, 1)

    loads[2].wait()
    build_tables()

    @pl.when(has[UP])
    def _():
        place_copy.wait_recv()

    beside_above = cols.astype(F32) < place_in[0:1, :]

    fill("obj_vl", jnp.where(beside_above, got("obj_ht"), obj[:, TOP, LEFT]))
    put("obj_vl")
    for k in CFG["R1post"]:
        put(*first[k])
    loads[3].wait()
    turn_probe()

    def put_stack(span_rows, span_cols, real, imag):
        for base, value in ((0, real), (3, imag)):
            high, low = split(value)
            for b, item in ((0, high), (1, low), (2, high)):
                stack[span_rows, pl.ds((base + b) * N + span_cols, item.shape[1])] = item

    def put_stack2(row, real, imag):
        for base, value in ((0, real), (3, imag)):
            high, low = split(value)
            for b, item in ((0, high), (1, low), (2, high)):
                stack2[pl.ds((base + b) * N + row, item.shape[0]), :] = item

    def exit_wave(half, quarter_left, quarter_right):
        span = TOP if half == 0 else BOTTOM
        for side, patch in ((0, quarter_left), (1, quarter_right)):
            lanes = pl.ds(side * W, W)
            pr, pi = probe[0, span, lanes], probe[1, span, lanes]
            put_stack(
                span, side * W,
                pr * patch[0] - pi * patch[1], pr * patch[1] + pi * patch[0],
            )

    def right_product(half):
        span = pl.ds(half * W, W)
        out = jnp.dot(stack[span, :], right_table[...], preferred_element_type=F32)
        put_stack2(half * W, out[:, :N], out[:, N:])

    def left_product(half):
        out = jnp.dot(
            left_table[pl.ds(half * N, N), :], stack2[...], preferred_element_type=F32
        )
        return out[:W], out[W:]

    def back_product(half):
        span = pl.ds(half * W, W)
        back_re, back_im = left_product(half)
        pr, pi = probe[0, span, :], probe[1, span, :]
        grad[0, span, :] = pr * back_re - pi * back_im
        grad[1, span, :] = -(pr * back_im) - pi * back_re

    def sweep(source, low_left, low_right, right_top, right_bottom):
        for k in CFG["sweep"]:
            if k == "t":
                top_right = jnp.where(below, low_right(), source[:, TOP, RIGHT])
                own = jnp.where(beside, right_top(), source[:, TOP, LEFT])
                exit_wave(0, jnp.where(below, low_left(), own), top_right)
                right_product(0)
            else:
                bottom = jnp.where(beside, right_bottom(), source[:, BOTTOM, LEFT])
                exit_wave(1, bottom, source[:, BOTTOM, RIGHT])
                right_product(1)
        for half in range(2):
            far_re, far_im = left_product(half)
            misfit = far_re * far_re + far_im * far_im - meas[pl.ds(half * W, W), :]
            put_stack(pl.ds(half * W, W), 0, misfit * far_re, -(misfit * far_im))
        for half in range(2):
            right_product(half)

    def update(old_obj, old_vel, new_obj, new_vel, span_r, span_c, gradient):
        speed = MOMENTUM * old_vel[:, span_r, span_c] + gradient
        moved = old_obj[:, span_r, span_c] - STEP * speed
        new_vel[:, span_r, span_c] = speed
        new_obj[:, span_r, span_c] = moved
        return moved

    loads[4].wait()
    sweep(
        obj, lambda: got("obj_vl"), lambda: got("obj_vr"),
        lambda: recv[SLOT["obj_ht"]], lambda: got("obj_hb"),
    )
    back_product(0)
    fill("grad_vl", jnp.where(below, grad[:, TOP, LEFT], 0.0))
    put("grad_vl")
    loads[5].wait()

    def coasting(span_r, span_c):
        return obj[:, span_r, span_c] - (STEP * MOMENTUM) * vel[:, span_r, span_c]

    def send_r():
        fill("grad_vr", jnp.where(below, grad[:, TOP, RIGHT], 0.0))
        put("grad_vr")

    def send_R():
        fill("next_vr", coasting(TOP, RIGHT) - STEP * jnp.where(below, 0.0, grad[:, TOP, RIGHT]))
        put("next_vr")

    def send_b():
        fill("grad_hb", jnp.where(beside, grad[:, BOTTOM, LEFT], 0.0))
        put("grad_hb")

    def send_B():
        fill("next_hb", coasting(BOTTOM, LEFT) - STEP * jnp.where(beside, 0.0, grad[:, BOTTOM, LEFT]))
        put("next_hb")

    sends = {"r": send_r, "R": send_R, "b": send_b, "B": send_B}
    for k in CFG["mid"]:
        if k == "|":
            back_product(1)
        else:
            sends[k]()

    above = got("grad_vl")
    across = jnp.where(beside & ~below, grad[:, TOP, LEFT], 0.0) + jnp.where(beside_above, above, 0.0)
    kept = jnp.where(below | beside, 0.0, grad[:, TOP, LEFT]) + jnp.where(beside_above, 0.0, above)
    halo[0] = across
    halo[1] = kept

    def send_h():
        fill("grad_ht", halo[0])
        put("grad_ht")

    def send_H():
        fill("next_ht", coasting(TOP, LEFT) - STEP * halo[1])
        put("next_ht")

    sends |= {"h": send_h, "H": send_H}
    for k in CFG["mid2"]:
        sends[k]()

    step_right = jnp.where(has[TO_RIGHT], STEP, 0.0)
    step_down = jnp.where(has[DOWN], STEP, 0.0)
    moving = (obj, vel, obj1, vel1)
    update(*moving, BOTTOM, RIGHT, grad[:, BOTTOM, RIGHT])
    moved = update(*moving, TOP, LEFT, halo[1] + got("grad_ht"))
    right_top = got("next_ht") - step_right * halo[0]
    halo[0] = right_top
    fill("next_vl", jnp.where(beside_above, right_top, moved))
    put("next_vl")
    update(*moving, BOTTOM, LEFT, jnp.where(beside, 0.0, grad[:, BOTTOM, LEFT]) + got("grad_hb"))
    update(*moving, TOP, RIGHT, jnp.where(below, 0.0, grad[:, TOP, RIGHT]) + got("grad_vr"))

    def low_right():
        return got("next_vr") - step_down * jnp.where(below, grad[:, TOP, RIGHT], 0.0)

    def right_bottom():
        return got("next_hb") - step_right * jnp.where(beside, grad[:, BOTTOM, LEFT], 0.0)

    sweep(obj1, lambda: got("next_vl"), low_right, lambda: halo[0], right_bottom)
    back_product(0)
    fill("last_vl", jnp.where(below, grad[:, TOP, LEFT], 0.0))
    put("last_vl")

    def last_r():
        fill("last_vr", jnp.where(below, grad[:, TOP, RIGHT], 0.0))
        put("last_vr")

    def last_b():
        fill("last_hb", jnp.where(beside, grad[:, BOTTOM, LEFT], 0.0))
        put("last_hb")

    lasts = {"r": last_r, "b": last_b, "|": lambda: back_product(1)}
    for k in CFG["R4pre"]:
        lasts[k]()
    above = got("last_vl")
    fill("last_ht", jnp.where(beside & ~below, grad[:, TOP, LEFT], 0.0) + jnp.where(beside_above, above, 0.0))
    put("last_ht")
    for k in CFG["R4post"]:
        lasts[k]()

    for there, copy in [started.pop(name) for name, _ in first.values()]:
        @pl.when(there)
        def _():
            copy.wait_send()

    stores = []
    moving = (obj1, vel1, obj, vel)

    def finish(span_r, span_c, gradient):
        update(*moving, span_r, span_c, gradient)
        for src, dst in ((obj, obj_out), (vel, vel_out)):
            copy = pltpu.make_async_copy(
                src.at[:, span_r, span_c], dst.at[:, span_r, span_c], store_sem.at[len(stores)]
            )
            copy.start()
            stores.append(copy)

    finish(BOTTOM, RIGHT, grad[:, BOTTOM, RIGHT])
    finish(TOP, RIGHT, jnp.where(below, 0.0, grad[:, TOP, RIGHT]) + got("last_vr"))
    kept = jnp.where(below | beside, 0.0, grad[:, TOP, LEFT]) + jnp.where(beside_above, 0.0, recv[SLOT["last_vl"]])
    if CFG["R4post"]:
        finish(TOP, LEFT, kept + got("last_ht"))
        finish(BOTTOM, LEFT, jnp.where(beside, 0.0, grad[:, BOTTOM, LEFT]) + got("last_hb"))
    else:
        finish(BOTTOM, LEFT, jnp.where(beside, 0.0, grad[:, BOTTOM, LEFT]) + got("last_hb"))
        finish(TOP, LEFT, kept + got("last_ht"))

    for there, copy in [*started.values(), (has[DOWN], place_copy)]:
        @pl.when(there)
        def _():
            copy.wait_send()

    for copy in stores:
        copy.wait()


def on_device(n_rows, n_cols, object_field, velocity, positions, measured, probe):
    vmem = lambda *shape: pltpu.VMEM(shape, F32)
    anywhere = pl.BlockSpec(memory_space=pl.ANY)
    count = len(MESSAGES)
    field = jax.ShapeDtypeStruct((2, N, N), F32)
    return pl.pallas_call(
        functools.partial(kernel, n_rows, n_cols),
        out_shape=(field, field),
        in_specs=[anywhere] * 6,
        out_specs=(anywhere, anywhere),
        scratch_shapes=[
            pltpu.SMEM((2,), jnp.int32),
            vmem(2, N, N), vmem(2, N, N), vmem(2, N, N), vmem(2, N, N),
            vmem(N, N), vmem(2, N, N),
            pltpu.VMEM((4, N, N), BF16),
            pltpu.VMEM((6 * N, 2 * N), BF16),
            pltpu.VMEM((2 * N, 6 * N), BF16),
            pltpu.VMEM((N, 6 * N), BF16),
            pltpu.VMEM((6 * N, N), BF16),
            vmem(2, N, N), vmem(2, 2, W, W),
            vmem(count, 2, W, W), vmem(count, 2, W, W),
            vmem(8, W), vmem(8, W),
            pltpu.SemaphoreType.DMA((6,)), pltpu.SemaphoreType.DMA((8,)),
            pltpu.SemaphoreType.DMA((count,)), pltpu.SemaphoreType.DMA((count,)),
            pltpu.SemaphoreType.DMA, pltpu.SemaphoreType.DMA,
        ],
        compiler_params=pltpu.CompilerParams(collective_id=0, has_side_effects=True),
        name="ptycho",
    )(
        positions.reshape(2), object_field, velocity, measured.reshape(N, N), probe,
        jnp.asarray(fourier_tables()),
    )


def solution(mesh):
    placed = (
        P(None, "row", "col"),
        P(None, "row", "col"),
        P("row", "col", None, None),
        P("row", "col", None, None, None),
        P(),
    )
    return jax.shard_map(
        functools.partial(on_device, mesh.shape["row"], mesh.shape["col"]),
        mesh=mesh,
        in_specs=placed,
        out_specs=(P(None, "row", "col"), P(None, "row", "col")),
        check_vma=False,
    )
```

```python
import functools
import re

import numpy as np

import jax
import jax.numpy as jnp
from jax import lax
from jax.experimental import pallas as pl
from jax.experimental.pallas import tpu as pltpu
from jax.sharding import PartitionSpec as P

N = 256
W = 128
ITERS = 2
STEP = 0.1
MOMENTUM = 0.8
MESH = pl.DeviceIdType.MESH
F32 = jnp.float32
BF16 = jnp.bfloat16

UP, DOWN, TO_LEFT, TO_RIGHT = (-1, 0), (1, 0), (0, -1), (0, 1)
MESSAGES = {
    "obj_ht": TO_LEFT, "obj_hb": TO_LEFT, "obj_vr": UP, "obj_vl": UP,
    "grad_vl": DOWN, "grad_vr": DOWN, "grad_hb": TO_RIGHT, "grad_ht": TO_RIGHT,
    "next_vr": UP, "next_hb": TO_LEFT, "next_ht": TO_LEFT, "next_vl": UP,
    "last_vl": DOWN, "last_vr": DOWN, "last_hb": TO_RIGHT, "last_ht": TO_RIGHT,
}
SLOT = {name: i for i, name in enumerate(MESSAGES)}
TOP, BOTTOM = pl.ds(0, W), pl.ds(W, W)
LEFT, RIGHT = pl.ds(0, W), pl.ds(W, W)


CFG = dict(R1pre="tb0r1b1", R1post="r0", mid="|bB", mid2="hHrR", R4pre="|r0b1", R4post="b0r1", sweep="bt")


def order(text):
    return [(k, int(p) if p else None) for k, p in re.findall(r"([a-zA-Z|])(\d?)", text)]


def fourier_tables():
    index = np.arange(N)
    angle = -2.0 * np.pi * (index[:, None] * index[None, :] % N) / N
    parts = []
    for table in (np.cos(angle) / np.sqrt(N), np.sin(angle) / np.sqrt(N)):
        high = table.astype(BF16)
        parts += [high, (table - high.astype(np.float64)).astype(BF16)]
    return np.stack(parts)


def split(value):
    high = value.astype(BF16)
    return high, (value - high.astype(F32)).astype(BF16)


def kernel(
    n_rows, n_cols,
    pos_hbm, obj_hbm, vel_hbm, meas_hbm, probe_hbm, table_hbm,
    obj_out, vel_out,
    pos, obj, vel, obj1, vel1, meas, probe, table, right_table, left_table,
    stack, stack2, grad, halo, recv, send, place, place_in,
    load_sem, send_sem, recv_sem, place_send, place_recv,
):
    r = lax.axis_index("row")
    c = lax.axis_index("col")
    has = {UP: r > 0, DOWN: r < n_rows - 1, TO_LEFT: c > 0, TO_RIGHT: c < n_cols - 1}

    barrier = pltpu.get_barrier_semaphore()
    for (dr, dc), there in has.items():
        @pl.when(there)
        def _():
            pl.semaphore_signal(barrier, inc=1, device_id=(r + dr, c + dc), device_id_type=MESH)

    loads = [
        pltpu.make_async_copy(src, dst, load_sem.at[i])
        for i, (src, dst) in enumerate([
            (pos_hbm, pos), (obj_hbm, obj), (table_hbm, table), (probe_hbm, probe),
            (meas_hbm, meas), (vel_hbm, vel),
        ])
    ]
    for load in loads:
        load.start()

    zeros = jnp.zeros((2, W, W), F32)
    for way in (UP, DOWN, TO_LEFT, TO_RIGHT):
        @pl.when(~has[-way[0], -way[1]])
        def _():
            for name, to in MESSAGES.items():
                if to == way:
                    recv[SLOT[name]] = zeros

    @pl.when(~has[UP])
    def _():
        place_in[...] = jnp.zeros((8, W), F32)

    with jax.named_scope("wait_barrier"):
        pl.semaphore_wait(barrier, sum(there.astype(jnp.int32) for there in has.values()))

    started = {}
    filled = set()

    def message(name, src):
        dr, dc = MESSAGES[name]
        i = SLOT[name]
        return pltpu.make_async_remote_copy(
            src_ref=src, dst_ref=recv.at[i], send_sem=send_sem.at[i], recv_sem=recv_sem.at[i],
            device_id=(r + dr, c + dc), device_id_type=MESH,
        )

    def put(name, src=None, only=None):
        copy = message(name, send.at[SLOT[name]] if src is None else src)
        there = has[MESSAGES[name]]

        @pl.when(there if only is None else there & (c % 2 == only))
        def _():
            copy.start()

        started[name] = there, copy

    def got(name):
        dr, dc = MESSAGES[name]
        with jax.named_scope("wait_" + name):
            @pl.when(has[-dr, -dc])
            def _():
                message(name, recv.at[SLOT[name]]).wait_recv()

        return recv[SLOT[name]]

    def fill(name, value):
        if name not in filled:
            filled.add(name)
            send[SLOT[name]] = value()

    place_copy = pltpu.make_async_remote_copy(
        src_ref=place, dst_ref=place_in, send_sem=place_send, recv_sem=place_recv,
        device_id=(r + 1, c), device_id_type=MESH,
    )
    with jax.named_scope("wait_load"):
        loads[1].wait()

    first = {
        "t": ("obj_ht", obj.at[:, TOP, LEFT]),
        "b": ("obj_hb", obj.at[:, BOTTOM, LEFT]),
        "r": ("obj_vr", obj.at[:, TOP, RIGHT]),
    }
    for k, only in order(CFG["R1pre"]):
        put(*first[k], only)

    loads[0].wait()
    dy = pos[0]
    dx = pos[1]
    rows = lax.broadcasted_iota(jnp.int32, (W, W), 0)
    cols = lax.broadcasted_iota(jnp.int32, (W, W), 1)
    below = rows < dy
    beside = cols < dx
    place[...] = jnp.full((8, W), dx.astype(F32))

    @pl.when(has[DOWN])
    def _():
        place_copy.start()

    def build_tables():
        re_high, re_low, im_high, im_low = (table[i] for i in range(4))
        blocks = [
            (re_high, im_high), (re_high, im_high), (re_low, im_low),
            (-im_high, re_high), (-im_high, re_high), (-im_low, re_low),
        ]
        for b, (real, imag) in enumerate(blocks):
            span = pl.ds(b * N, N)
            right_table[span, pl.ds(0, N)] = real
            right_table[span, pl.ds(N, N)] = imag
            for half in range(2):
                left_table[pl.ds(half * N, W), span] = real[half * W : (half + 1) * W]
                left_table[pl.ds(half * N + W, W), span] = imag[half * W : (half + 1) * W]

    def turn_probe():
        for part in range(2):
            turned = pltpu.roll(probe[part], dy, 0)
            probe[part] = pltpu.roll(turned, dx, 1)

    loads[2].wait()
    build_tables()

    @pl.when(has[UP])
    def _():
        place_copy.wait_recv()

    beside_above = cols.astype(F32) < place_in[0:1, :]

    fill("obj_vl", lambda: jnp.where(beside_above, got("obj_ht"), obj[:, TOP, LEFT]))
    put("obj_vl")
    for k, only in order(CFG["R1post"]):
        put(*first[k], only)
    loads[3].wait()
    turn_probe()

    def put_stack(span_rows, span_cols, real, imag):
        for base, value in ((0, real), (3, imag)):
            high, low = split(value)
            for b, item in ((0, high), (1, low), (2, high)):
                stack[span_rows, pl.ds((base + b) * N + span_cols, item.shape[1])] = item

    def put_stack2(row, real, imag):
        for base, value in ((0, real), (3, imag)):
            high, low = split(value)
            for b, item in ((0, high), (1, low), (2, high)):
                stack2[pl.ds((base + b) * N + row, item.shape[0]), :] = item

    def exit_wave(half, quarter_left, quarter_right):
        span = TOP if half == 0 else BOTTOM
        for side, patch in ((0, quarter_left), (1, quarter_right)):
            lanes = pl.ds(side * W, W)
            pr, pi = probe[0, span, lanes], probe[1, span, lanes]
            put_stack(
                span, side * W,
                pr * patch[0] - pi * patch[1], pr * patch[1] + pi * patch[0],
            )

    def right_product(half):
        span = pl.ds(half * W, W)
        out = jnp.dot(stack[span, :], right_table[...], preferred_element_type=F32)
        put_stack2(half * W, out[:, :N], out[:, N:])

    def left_product(half):
        out = jnp.dot(
            left_table[pl.ds(half * N, N), :], stack2[...], preferred_element_type=F32
        )
        return out[:W], out[W:]

    def back_product(half):
        span = pl.ds(half * W, W)
        back_re, back_im = left_product(half)
        pr, pi = probe[0, span, :], probe[1, span, :]
        grad[0, span, :] = pr * back_re - pi * back_im
        grad[1, span, :] = -(pr * back_im) - pi * back_re

    def sweep(source, low_left, low_right, right_top, right_bottom):
        for k in CFG["sweep"]:
            if k == "t":
                top_right = jnp.where(below, low_right(), source[:, TOP, RIGHT])
                own = jnp.where(beside, right_top(), source[:, TOP, LEFT])
                exit_wave(0, jnp.where(below, low_left(), own), top_right)
                right_product(0)
            else:
                bottom = jnp.where(beside, right_bottom(), source[:, BOTTOM, LEFT])
                exit_wave(1, bottom, source[:, BOTTOM, RIGHT])
                right_product(1)
        for half in range(2):
            far_re, far_im = left_product(half)
            misfit = far_re * far_re + far_im * far_im - meas[pl.ds(half * W, W), :]
            put_stack(pl.ds(half * W, W), 0, misfit * far_re, -(misfit * far_im))
        for half in range(2):
            right_product(half)

    def update(old_obj, old_vel, new_obj, new_vel, span_r, span_c, gradient):
        speed = MOMENTUM * old_vel[:, span_r, span_c] + gradient
        moved = old_obj[:, span_r, span_c] - STEP * speed
        new_vel[:, span_r, span_c] = speed
        new_obj[:, span_r, span_c] = moved
        return moved

    loads[4].wait()
    sweep(
        obj, lambda: got("obj_vl"), lambda: got("obj_vr"),
        lambda: recv[SLOT["obj_ht"]], lambda: got("obj_hb"),
    )
    back_product(0)
    fill("grad_vl", lambda: jnp.where(below, grad[:, TOP, LEFT], 0.0))
    put("grad_vl")
    loads[5].wait()

    def coasting(span_r, span_c):
        return obj[:, span_r, span_c] - (STEP * MOMENTUM) * vel[:, span_r, span_c]

    def send_r(only):
        fill("grad_vr", lambda: jnp.where(below, grad[:, TOP, RIGHT], 0.0))
        put("grad_vr", only=only)

    def send_R(only):
        fill("next_vr", lambda: coasting(TOP, RIGHT) - STEP * jnp.where(below, 0.0, grad[:, TOP, RIGHT]))
        put("next_vr", only=only)

    def send_b(only):
        fill("grad_hb", lambda: jnp.where(beside, grad[:, BOTTOM, LEFT], 0.0))
        put("grad_hb", only=only)

    def send_B(only):
        fill("next_hb", lambda: coasting(BOTTOM, LEFT) - STEP * jnp.where(beside, 0.0, grad[:, BOTTOM, LEFT]))
        put("next_hb", only=only)

    sends = {"r": send_r, "R": send_R, "b": send_b, "B": send_B}
    for k, only in order(CFG["mid"]):
        if k == "|":
            back_product(1)
        else:
            sends[k](only)

    above = got("grad_vl")
    across = jnp.where(beside & ~below, grad[:, TOP, LEFT], 0.0) + jnp.where(beside_above, above, 0.0)
    kept = jnp.where(below | beside, 0.0, grad[:, TOP, LEFT]) + jnp.where(beside_above, 0.0, above)
    halo[0] = across
    halo[1] = kept

    def send_h(only):
        fill("grad_ht", lambda: halo[0])
        put("grad_ht", only=only)

    def send_H(only):
        fill("next_ht", lambda: coasting(TOP, LEFT) - STEP * halo[1])
        put("next_ht", only=only)

    sends |= {"h": send_h, "H": send_H}
    for k, only in order(CFG["mid2"]):
        sends[k](only)

    step_right = jnp.where(has[TO_RIGHT], STEP, 0.0)
    step_down = jnp.where(has[DOWN], STEP, 0.0)
    moving = (obj, vel, obj1, vel1)
    update(*moving, BOTTOM, RIGHT, grad[:, BOTTOM, RIGHT])
    moved = update(*moving, TOP, LEFT, halo[1] + got("grad_ht"))
    right_top = got("next_ht") - step_right * halo[0]
    halo[0] = right_top
    fill("next_vl", lambda: jnp.where(beside_above, right_top, moved))
    put("next_vl")
    update(*moving, BOTTOM, LEFT, jnp.where(beside, 0.0, grad[:, BOTTOM, LEFT]) + got("grad_hb"))
    update(*moving, TOP, RIGHT, jnp.where(below, 0.0, grad[:, TOP, RIGHT]) + got("grad_vr"))

    def low_right():
        return got("next_vr") - step_down * jnp.where(below, grad[:, TOP, RIGHT], 0.0)

    def right_bottom():
        return got("next_hb") - step_right * jnp.where(beside, grad[:, BOTTOM, LEFT], 0.0)

    sweep(obj1, lambda: got("next_vl"), low_right, lambda: halo[0], right_bottom)
    back_product(0)
    fill("last_vl", lambda: jnp.where(below, grad[:, TOP, LEFT], 0.0))
    put("last_vl")

    def last_r(only):
        fill("last_vr", lambda: jnp.where(below, grad[:, TOP, RIGHT], 0.0))
        put("last_vr", only=only)

    def last_b(only):
        fill("last_hb", lambda: jnp.where(beside, grad[:, BOTTOM, LEFT], 0.0))
        put("last_hb", only=only)

    lasts = {"r": last_r, "b": last_b, "|": lambda only: back_product(1)}
    for k, only in order(CFG["R4pre"]):
        lasts[k](only)
    above = got("last_vl")
    fill("last_ht", lambda: jnp.where(beside & ~below, grad[:, TOP, LEFT], 0.0) + jnp.where(beside_above, above, 0.0))
    put("last_ht")
    for k, only in order(CFG["R4post"]):
        lasts[k](only)

    moving = (obj1, vel1, obj_out, vel_out)

    def finish(span_r, span_c, gradient):
        update(*moving, span_r, span_c, gradient)

    finish(BOTTOM, RIGHT, grad[:, BOTTOM, RIGHT])
    finish(TOP, RIGHT, jnp.where(below, 0.0, grad[:, TOP, RIGHT]) + got("last_vr"))
    kept = jnp.where(below | beside, 0.0, grad[:, TOP, LEFT]) + jnp.where(beside_above, 0.0, recv[SLOT["last_vl"]])
    if CFG["R4post"]:
        finish(TOP, LEFT, kept + got("last_ht"))
        finish(BOTTOM, LEFT, jnp.where(beside, 0.0, grad[:, BOTTOM, LEFT]) + got("last_hb"))
    else:
        finish(BOTTOM, LEFT, jnp.where(beside, 0.0, grad[:, BOTTOM, LEFT]) + got("last_hb"))
        finish(TOP, LEFT, kept + got("last_ht"))

    for there, copy in [*started.values(), (has[DOWN], place_copy)]:
        @pl.when(there)
        def _():
            copy.wait_send()


def write_kernel(obj, vel, obj_out, vel_out, sem):
    copies = [
        pltpu.make_async_copy(src.at[part], dst.at[part], sem.at[2 * i + part])
        for i, (src, dst) in enumerate([(obj, obj_out), (vel, vel_out)])
        for part in range(2)
    ]
    for copy in copies:
        copy.start()
    for copy in copies:
        copy.wait()


def on_device(n_rows, n_cols, object_field, velocity, positions, measured, probe):
    vmem = lambda *shape: pltpu.VMEM(shape, F32)
    anywhere = pl.BlockSpec(memory_space=pl.ANY)
    count = len(MESSAGES)
    results = pl.pallas_call(
        functools.partial(kernel, n_rows, n_cols),
        out_shape=(pltpu.VMEM((2, N, N), F32), pltpu.VMEM((2, N, N), F32)),
        in_specs=[anywhere] * 6,
        out_specs=(pl.BlockSpec(memory_space=pltpu.VMEM),) * 2,
        scratch_shapes=[
            pltpu.SMEM((2,), jnp.int32),
            vmem(2, N, N), vmem(2, N, N), vmem(2, N, N), vmem(2, N, N),
            vmem(N, N), vmem(2, N, N),
            pltpu.VMEM((4, N, N), BF16),
            pltpu.VMEM((6 * N, 2 * N), BF16),
            pltpu.VMEM((2 * N, 6 * N), BF16),
            pltpu.VMEM((N, 6 * N), BF16),
            pltpu.VMEM((6 * N, N), BF16),
            vmem(2, N, N), vmem(2, 2, W, W),
            vmem(count, 2, W, W), vmem(count, 2, W, W),
            vmem(8, W), vmem(8, W),
            pltpu.SemaphoreType.DMA((6,)),
            pltpu.SemaphoreType.DMA((count,)), pltpu.SemaphoreType.DMA((count,)),
            pltpu.SemaphoreType.DMA, pltpu.SemaphoreType.DMA,
        ],
        compiler_params=pltpu.CompilerParams(collective_id=0, has_side_effects=True),
        name="ptycho",
    )(
        positions.reshape(2), object_field, velocity, measured.reshape(N, N), probe,
        jnp.asarray(fourier_tables()),
    )
    field = jax.ShapeDtypeStruct((2, N, N), F32)
    return pl.pallas_call(
        write_kernel,
        out_shape=(field, field),
        in_specs=[pl.BlockSpec(memory_space=pltpu.VMEM)] * 2,
        out_specs=(anywhere, anywhere),
        scratch_shapes=[pltpu.SemaphoreType.DMA((4,))],
        name="write",
    )(*(pltpu.with_memory_space_constraint(x, pltpu.VMEM) for x in results))


def solution(mesh):
    placed = (
        P(None, "row", "col"),
        P(None, "row", "col"),
        P("row", "col", None, None),
        P("row", "col", None, None, None),
        P(),
    )
    return jax.shard_map(
        functools.partial(on_device, mesh.shape["row"], mesh.shape["col"]),
        mesh=mesh,
        in_specs=placed,
        out_specs=(P(None, "row", "col"), P(None, "row", "col")),
        check_vma=False,
    )
```

```python
import functools
import re

import numpy as np

import jax
import jax.numpy as jnp
from jax import lax
from jax.experimental import pallas as pl
from jax.experimental.pallas import tpu as pltpu
from jax.sharding import PartitionSpec as P

N = 256
W = 128
ITERS = 2
STEP = 0.1
MOMENTUM = 0.8
MESH = pl.DeviceIdType.MESH
F32 = jnp.float32
BF16 = jnp.bfloat16

UP, DOWN, TO_LEFT, TO_RIGHT = (-1, 0), (1, 0), (0, -1), (0, 1)
MESSAGES = {
    "obj_ht": TO_LEFT, "obj_hb": TO_LEFT, "obj_vr": UP, "obj_vl": UP,
    "grad_vl": DOWN, "grad_vr": DOWN, "grad_hb": TO_RIGHT, "grad_ht": TO_RIGHT,
    "next_vr": UP, "next_hb": TO_LEFT, "next_ht": TO_LEFT, "next_vl": UP,
    "last_vl": DOWN, "last_vr": DOWN, "last_hb": TO_RIGHT, "last_ht": TO_RIGHT,
}
SLOT = {name: i for i, name in enumerate(MESSAGES)}
TOP, BOTTOM = pl.ds(0, W), pl.ds(W, W)
LEFT, RIGHT = pl.ds(0, W), pl.ds(W, W)


CFG = dict(R1pre="tb0r1b1", R1post="r0", mid="|bB", mid2="hHw1rR", R4pre="|r0b1", R4post="b0r1", sweep="bt", R1x=())


def order(text):
    return [(k, int(p) if p else None) for k, p in re.findall(r"([a-zA-Z|])(\d?)", text)]


def fourier_tables():
    index = np.arange(N)
    angle = -2.0 * np.pi * (index[:, None] * index[None, :] % N) / N
    parts = []
    for table in (np.cos(angle) / np.sqrt(N), np.sin(angle) / np.sqrt(N)):
        high = table.astype(BF16)
        parts += [high, (table - high.astype(np.float64)).astype(BF16)]
    return np.stack(parts)


def split(value):
    high = value.astype(BF16)
    return high, (value - high.astype(F32)).astype(BF16)


def kernel(
    n_rows, n_cols,
    pos_hbm, obj_hbm, vel_hbm, meas_hbm, probe_hbm, table_hbm,
    obj_out, vel_out,
    pos, obj, vel, obj1, vel1, meas, probe, table, right_table, left_table,
    stack, stack2, grad, halo, recv, send, place, place_in,
    load_sem, send_sem, recv_sem, place_send, place_recv,
):
    r = lax.axis_index("row")
    c = lax.axis_index("col")
    has = {UP: r > 0, DOWN: r < n_rows - 1, TO_LEFT: c > 0, TO_RIGHT: c < n_cols - 1}

    barrier = pltpu.get_barrier_semaphore()
    for (dr, dc), there in has.items():
        @pl.when(there)
        def _():
            pl.semaphore_signal(barrier, inc=1, device_id=(r + dr, c + dc), device_id_type=MESH)

    loads = [
        pltpu.make_async_copy(src, dst, load_sem.at[i])
        for i, (src, dst) in enumerate([
            (pos_hbm, pos), (obj_hbm, obj), (table_hbm, table), (probe_hbm, probe),
            (meas_hbm, meas), (vel_hbm, vel),
        ])
    ]
    for load in loads:
        load.start()

    zeros = jnp.zeros((2, W, W), F32)
    for way in (UP, DOWN, TO_LEFT, TO_RIGHT):
        @pl.when(~has[-way[0], -way[1]])
        def _():
            for name, to in MESSAGES.items():
                if to == way:
                    recv[SLOT[name]] = zeros

    @pl.when(~has[UP])
    def _():
        place_in[...] = jnp.zeros((8, W), F32)

    with jax.named_scope("wait_barrier"):
        pl.semaphore_wait(barrier, sum(there.astype(jnp.int32) for there in has.values()))

    started = {}
    filled = set()
    flushed = {}

    def message(name, src):
        dr, dc = MESSAGES[name]
        i = SLOT[name]
        return pltpu.make_async_remote_copy(
            src_ref=src, dst_ref=recv.at[i], send_sem=send_sem.at[i], recv_sem=recv_sem.at[i],
            device_id=(r + dr, c + dc), device_id_type=MESH,
        )

    def put(name, src=None, only=None):
        copy = message(name, send.at[SLOT[name]] if src is None else src)
        there = has[MESSAGES[name]]

        @pl.when(there if only is None else there & (c % 2 == only))
        def _():
            copy.start()

        started[name] = there, copy

    def flush(name, only):
        there, copy = started[name]
        flushed[name] = only

        @pl.when(there & (c % 2 == only))
        def _():
            copy.wait_send()

    def got(name):
        dr, dc = MESSAGES[name]
        with jax.named_scope("wait_" + name):
            @pl.when(has[-dr, -dc])
            def _():
                message(name, recv.at[SLOT[name]]).wait_recv()

        return recv[SLOT[name]]

    def fill(name, value):
        if name not in filled:
            filled.add(name)
            send[SLOT[name]] = value()

    place_copy = pltpu.make_async_remote_copy(
        src_ref=place, dst_ref=place_in, send_sem=place_send, recv_sem=place_recv,
        device_id=(r + 1, c), device_id_type=MESH,
    )
    with jax.named_scope("wait_load"):
        loads[1].wait()

    first = {
        "t": ("obj_ht", obj.at[:, TOP, LEFT]),
        "b": ("obj_hb", obj.at[:, BOTTOM, LEFT]),
        "r": ("obj_vr", obj.at[:, TOP, RIGHT]),
    }
    for k, only in order(CFG["R1pre"]):
        put(*first[k], only)

    loads[0].wait()
    dy = pos[0]
    dx = pos[1]
    rows = lax.broadcasted_iota(jnp.int32, (W, W), 0)
    cols = lax.broadcasted_iota(jnp.int32, (W, W), 1)
    below = rows < dy
    beside = cols < dx
    place[...] = jnp.full((8, W), dx.astype(F32))

    @pl.when(has[DOWN])
    def _():
        place_copy.start()

    def build_tables():
        re_high, re_low, im_high, im_low = (table[i] for i in range(4))
        blocks = [
            (re_high, im_high), (re_high, im_high), (re_low, im_low),
            (-im_high, re_high), (-im_high, re_high), (-im_low, re_low),
        ]
        for b, (real, imag) in enumerate(blocks):
            span = pl.ds(b * N, N)
            right_table[span, pl.ds(0, N)] = real
            right_table[span, pl.ds(N, N)] = imag
            for half in range(2):
                left_table[pl.ds(half * N, W), span] = real[half * W : (half + 1) * W]
                left_table[pl.ds(half * N + W, W), span] = imag[half * W : (half + 1) * W]

    def turn_probe():
        for part in range(2):
            turned = pltpu.roll(probe[part], dy, 0)
            probe[part] = pltpu.roll(turned, dx, 1)

    loads[2].wait()
    build_tables()

    @pl.when(has[UP])
    def _():
        place_copy.wait_recv()

    beside_above = cols.astype(F32) < place_in[0:1, :]

    for name in CFG["R1x"]:
        flush(name, 0)

    fill("obj_vl", lambda: jnp.where(beside_above, got("obj_ht"), obj[:, TOP, LEFT]))
    put("obj_vl")
    for k, only in order(CFG["R1post"]):
        put(*first[k], only)
    loads[3].wait()
    turn_probe()

    def put_stack(span_rows, span_cols, real, imag):
        for base, value in ((0, real), (3, imag)):
            high, low = split(value)
            for b, item in ((0, high), (1, low), (2, high)):
                stack[span_rows, pl.ds((base + b) * N + span_cols, item.shape[1])] = item

    def put_stack2(row, real, imag):
        for base, value in ((0, real), (3, imag)):
            high, low = split(value)
            for b, item in ((0, high), (1, low), (2, high)):
                stack2[pl.ds((base + b) * N + row, item.shape[0]), :] = item

    def exit_wave(half, quarter_left, quarter_right):
        span = TOP if half == 0 else BOTTOM
        for side, patch in ((0, quarter_left), (1, quarter_right)):
            lanes = pl.ds(side * W, W)
            pr, pi = probe[0, span, lanes], probe[1, span, lanes]
            put_stack(
                span, side * W,
                pr * patch[0] - pi * patch[1], pr * patch[1] + pi * patch[0],
            )

    def right_product(half):
        span = pl.ds(half * W, W)
        out = jnp.dot(stack[span, :], right_table[...], preferred_element_type=F32)
        put_stack2(half * W, out[:, :N], out[:, N:])

    def left_product(half):
        out = jnp.dot(
            left_table[pl.ds(half * N, N), :], stack2[...], preferred_element_type=F32
        )
        return out[:W], out[W:]

    def back_product(half):
        span = pl.ds(half * W, W)
        back_re, back_im = left_product(half)
        pr, pi = probe[0, span, :], probe[1, span, :]
        grad[0, span, :] = pr * back_re - pi * back_im
        grad[1, span, :] = -(pr * back_im) - pi * back_re

    def sweep(source, low_left, low_right, right_top, right_bottom):
        for k in CFG["sweep"]:
            if k == "t":
                top_right = jnp.where(below, low_right(), source[:, TOP, RIGHT])
                own = jnp.where(beside, right_top(), source[:, TOP, LEFT])
                exit_wave(0, jnp.where(below, low_left(), own), top_right)
                right_product(0)
            else:
                bottom = jnp.where(beside, right_bottom(), source[:, BOTTOM, LEFT])
                exit_wave(1, bottom, source[:, BOTTOM, RIGHT])
                right_product(1)
        for half in range(2):
            far_re, far_im = left_product(half)
            misfit = far_re * far_re + far_im * far_im - meas[pl.ds(half * W, W), :]
            put_stack(pl.ds(half * W, W), 0, misfit * far_re, -(misfit * far_im))
        for part in range(2):
            out = jnp.dot(
                stack[...], right_table[:, pl.ds(part * N, N)], preferred_element_type=F32
            )
            high, low = split(out)
            for b, item in ((0, high), (1, low), (2, high)):
                stack2[pl.ds((3 * part + b) * N, N), :] = item

    def update(old_obj, old_vel, new_obj, new_vel, span_r, span_c, gradient):
        speed = MOMENTUM * old_vel[:, span_r, span_c] + gradient
        moved = old_obj[:, span_r, span_c] - STEP * speed
        new_vel[:, span_r, span_c] = speed
        new_obj[:, span_r, span_c] = moved
        return moved

    loads[4].wait()
    sweep(
        obj, lambda: got("obj_vl"), lambda: got("obj_vr"),
        lambda: recv[SLOT["obj_ht"]], lambda: got("obj_hb"),
    )
    back_product(0)
    fill("grad_vl", lambda: jnp.where(below, grad[:, TOP, LEFT], 0.0))
    put("grad_vl")
    loads[5].wait()

    def coasting(span_r, span_c):
        return obj[:, span_r, span_c] - (STEP * MOMENTUM) * vel[:, span_r, span_c]

    def send_r(only):
        fill("grad_vr", lambda: jnp.where(below, grad[:, TOP, RIGHT], 0.0))
        put("grad_vr", only=only)

    def send_R(only):
        fill("next_vr", lambda: coasting(TOP, RIGHT) - STEP * jnp.where(below, 0.0, grad[:, TOP, RIGHT]))
        put("next_vr", only=only)

    def send_b(only):
        fill("grad_hb", lambda: jnp.where(beside, grad[:, BOTTOM, LEFT], 0.0))
        put("grad_hb", only=only)

    def send_B(only):
        fill("next_hb", lambda: coasting(BOTTOM, LEFT) - STEP * jnp.where(beside, 0.0, grad[:, BOTTOM, LEFT]))
        put("next_hb", only=only)

    sends = {"r": send_r, "R": send_R, "b": send_b, "B": send_B}
    for k, only in order(CFG["mid"]):
        if k == "|":
            back_product(1)
        else:
            sends[k](only)

    above = got("grad_vl")
    across = jnp.where(beside & ~below, grad[:, TOP, LEFT], 0.0) + jnp.where(beside_above, above, 0.0)
    kept = jnp.where(below | beside, 0.0, grad[:, TOP, LEFT]) + jnp.where(beside_above, 0.0, above)
    halo[0] = across
    halo[1] = kept

    def send_h(only):
        fill("grad_ht", lambda: halo[0])
        put("grad_ht", only=only)

    def send_H(only):
        fill("next_ht", lambda: coasting(TOP, LEFT) - STEP * halo[1])
        put("next_ht", only=only)

    sends |= {
        "h": send_h, "H": send_H,
        "w": lambda only: flush("grad_ht", only), "W": lambda only: flush("next_ht", only),
    }
    for k, only in order(CFG["mid2"]):
        sends[k](only)

    step_right = jnp.where(has[TO_RIGHT], STEP, 0.0)
    step_down = jnp.where(has[DOWN], STEP, 0.0)
    moving = (obj, vel, obj1, vel1)
    update(*moving, BOTTOM, RIGHT, grad[:, BOTTOM, RIGHT])
    moved = update(*moving, TOP, LEFT, halo[1] + got("grad_ht"))
    right_top = got("next_ht") - step_right * halo[0]
    halo[0] = right_top
    fill("next_vl", lambda: jnp.where(beside_above, right_top, moved))
    put("next_vl")
    update(*moving, BOTTOM, LEFT, jnp.where(beside, 0.0, grad[:, BOTTOM, LEFT]) + got("grad_hb"))

    def low_right():
        update(*moving, TOP, RIGHT, jnp.where(below, 0.0, grad[:, TOP, RIGHT]) + got("grad_vr"))
        return got("next_vr") - step_down * jnp.where(below, grad[:, TOP, RIGHT], 0.0)

    def right_bottom():
        return got("next_hb") - step_right * jnp.where(beside, grad[:, BOTTOM, LEFT], 0.0)

    sweep(obj1, lambda: got("next_vl"), low_right, lambda: halo[0], right_bottom)
    back_product(0)
    fill("last_vl", lambda: jnp.where(below, grad[:, TOP, LEFT], 0.0))
    put("last_vl")

    def last_r(only):
        fill("last_vr", lambda: jnp.where(below, grad[:, TOP, RIGHT], 0.0))
        put("last_vr", only=only)

    def last_b(only):
        fill("last_hb", lambda: jnp.where(beside, grad[:, BOTTOM, LEFT], 0.0))
        put("last_hb", only=only)

    lasts = {"r": last_r, "b": last_b, "|": lambda only: back_product(1)}
    for k, only in order(CFG["R4pre"]):
        lasts[k](only)
    above = got("last_vl")
    fill("last_ht", lambda: jnp.where(beside & ~below, grad[:, TOP, LEFT], 0.0) + jnp.where(beside_above, above, 0.0))
    put("last_ht")
    for k, only in order(CFG["R4post"]):
        lasts[k](only)

    moving = (obj1, vel1, obj_out, vel_out)

    def finish(span_r, span_c, gradient):
        update(*moving, span_r, span_c, gradient)

    finish(BOTTOM, RIGHT, grad[:, BOTTOM, RIGHT])
    finish(TOP, RIGHT, jnp.where(below, 0.0, grad[:, TOP, RIGHT]) + got("last_vr"))
    kept = jnp.where(below | beside, 0.0, grad[:, TOP, LEFT]) + jnp.where(beside_above, 0.0, recv[SLOT["last_vl"]])
    if CFG["R4post"]:
        finish(TOP, LEFT, kept + got("last_ht"))
        finish(BOTTOM, LEFT, jnp.where(beside, 0.0, grad[:, BOTTOM, LEFT]) + got("last_hb"))
    else:
        finish(BOTTOM, LEFT, jnp.where(beside, 0.0, grad[:, BOTTOM, LEFT]) + got("last_hb"))
        finish(TOP, LEFT, kept + got("last_ht"))

    for name, (there, copy) in started.items():
        @pl.when(there & (c % 2 != flushed[name]) if name in flushed else there)
        def _():
            copy.wait_send()

    @pl.when(has[DOWN])
    def _():
        place_copy.wait_send()


def write_kernel(obj, vel, obj_out, vel_out, sem):
    copies = [
        pltpu.make_async_copy(src.at[part], dst.at[part], sem.at[2 * i + part])
        for i, (src, dst) in enumerate([(obj, obj_out), (vel, vel_out)])
        for part in range(2)
    ]
    for copy in copies:
        copy.start()
    for copy in copies:
        copy.wait()


def on_device(n_rows, n_cols, object_field, velocity, positions, measured, probe):
    vmem = lambda *shape: pltpu.VMEM(shape, F32)
    anywhere = pl.BlockSpec(memory_space=pl.ANY)
    count = len(MESSAGES)
    results = pl.pallas_call(
        functools.partial(kernel, n_rows, n_cols),
        out_shape=(pltpu.VMEM((2, N, N), F32), pltpu.VMEM((2, N, N), F32)),
        in_specs=[anywhere] * 6,
        out_specs=(pl.BlockSpec(memory_space=pltpu.VMEM),) * 2,
        scratch_shapes=[
            pltpu.SMEM((2,), jnp.int32),
            vmem(2, N, N), vmem(2, N, N), vmem(2, N, N), vmem(2, N, N),
            vmem(N, N), vmem(2, N, N),
            pltpu.VMEM((4, N, N), BF16),
            pltpu.VMEM((6 * N, 2 * N), BF16),
            pltpu.VMEM((2 * N, 6 * N), BF16),
            pltpu.VMEM((N, 6 * N), BF16),
            pltpu.VMEM((6 * N, N), BF16),
            vmem(2, N, N), vmem(2, 2, W, W),
            vmem(count, 2, W, W), vmem(count, 2, W, W),
            vmem(8, W), vmem(8, W),
            pltpu.SemaphoreType.DMA((6,)),
            pltpu.SemaphoreType.DMA((count,)), pltpu.SemaphoreType.DMA((count,)),
            pltpu.SemaphoreType.DMA, pltpu.SemaphoreType.DMA,
        ],
        compiler_params=pltpu.CompilerParams(collective_id=0, has_side_effects=True),
        name="ptycho",
    )(
        positions.reshape(2), object_field, velocity, measured.reshape(N, N), probe,
        jnp.asarray(fourier_tables()),
    )
    field = jax.ShapeDtypeStruct((2, N, N), F32)
    return pl.pallas_call(
        write_kernel,
        out_shape=(field, field),
        in_specs=[pl.BlockSpec(memory_space=pltpu.VMEM)] * 2,
        out_specs=(anywhere, anywhere),
        scratch_shapes=[pltpu.SemaphoreType.DMA((4,))],
        name="write",
    )(*(pltpu.with_memory_space_constraint(x, pltpu.VMEM) for x in results))


def solution(mesh):
    placed = (
        P(None, "row", "col"),
        P(None, "row", "col"),
        P("row", "col", None, None),
        P("row", "col", None, None, None),
        P(),
    )
    return jax.shard_map(
        functools.partial(on_device, mesh.shape["row"], mesh.shape["col"]),
        mesh=mesh,
        in_specs=placed,
        out_specs=(P(None, "row", "col"), P(None, "row", "col")),
        check_vma=False,
    )
```

```python
import functools
import re

import numpy as np

import jax
import jax.numpy as jnp
from jax import lax
from jax.experimental import pallas as pl
from jax.experimental.pallas import tpu as pltpu
from jax.sharding import PartitionSpec as P

N = 256
W = 128
ITERS = 2
STEP = 0.1
MOMENTUM = 0.8
MESH = pl.DeviceIdType.MESH
F32 = jnp.float32
BF16 = jnp.bfloat16

UP, DOWN, TO_LEFT, TO_RIGHT = (-1, 0), (1, 0), (0, -1), (0, 1)
MESSAGES = {
    "obj_ht": TO_LEFT, "obj_hb": TO_LEFT, "obj_vr": UP, "obj_vl": UP,
    "grad_vl": DOWN, "grad_vr": DOWN, "grad_hb": TO_RIGHT, "grad_ht": TO_RIGHT,
    "next_vr": UP, "next_hb": TO_LEFT, "next_ht": TO_LEFT, "next_vl": UP,
    "last_vl": DOWN, "last_vr": DOWN, "last_hb": TO_RIGHT, "last_ht": TO_RIGHT,
}
SLOT = {name: i for i, name in enumerate(MESSAGES)}
TOP, BOTTOM = pl.ds(0, W), pl.ds(W, W)
LEFT, RIGHT = pl.ds(0, W), pl.ds(W, W)


CFG = dict(R1pre="tb0r1b1", R1post="r0", mid="|bB", mid2="hHw1W0rR", R4pre="|r0b1", R4post="b0r1", sweep="bt", R1x=("obj_ht", "obj_hb"))


def order(text):
    return [(k, int(p) if p else None) for k, p in re.findall(r"([a-zA-Z|])(\d?)", text)]


def fourier_tables():
    index = np.arange(N)
    angle = -2.0 * np.pi * (index[:, None] * index[None, :] % N) / N
    parts = []
    for table in (np.cos(angle) / np.sqrt(N), np.sin(angle) / np.sqrt(N)):
        high = table.astype(BF16)
        parts += [high, (table - high.astype(np.float64)).astype(BF16)]
    return np.stack(parts)


def split(value):
    high = value.astype(BF16)
    return high, (value - high.astype(F32)).astype(BF16)


def kernel(
    n_rows, n_cols,
    pos_hbm, obj_hbm, vel_hbm, meas_hbm, probe_hbm, table_hbm,
    obj_out, vel_out,
    pos, obj, vel, obj1, vel1, meas, probe, table, right_table, left_table,
    stack, stack2, grad, halo, recv, send, place, place_in,
    load_sem, send_sem, recv_sem, place_send, place_recv,
):
    r = lax.axis_index("row")
    c = lax.axis_index("col")
    has = {UP: r > 0, DOWN: r < n_rows - 1, TO_LEFT: c > 0, TO_RIGHT: c < n_cols - 1}

    barrier = pltpu.get_barrier_semaphore()
    for (dr, dc), there in has.items():
        @pl.when(there)
        def _():
            pl.semaphore_signal(barrier, inc=1, device_id=(r + dr, c + dc), device_id_type=MESH)

    loads = [
        pltpu.make_async_copy(src, dst, load_sem.at[i])
        for i, (src, dst) in enumerate([
            (pos_hbm, pos), (obj_hbm, obj), (table_hbm, table), (probe_hbm, probe),
            (meas_hbm, meas), (vel_hbm, vel),
        ])
    ]
    for load in loads:
        load.start()

    zeros = jnp.zeros((2, W, W), F32)
    for way in (UP, DOWN, TO_LEFT, TO_RIGHT):
        @pl.when(~has[-way[0], -way[1]])
        def _():
            for name, to in MESSAGES.items():
                if to == way:
                    recv[SLOT[name]] = zeros

    @pl.when(~has[UP])
    def _():
        place_in[...] = jnp.zeros((8, W), F32)

    with jax.named_scope("wait_barrier"):
        pl.semaphore_wait(barrier, sum(there.astype(jnp.int32) for there in has.values()))

    started = {}
    filled = set()
    flushed = {}

    def message(name, src):
        dr, dc = MESSAGES[name]
        i = SLOT[name]
        return pltpu.make_async_remote_copy(
            src_ref=src, dst_ref=recv.at[i], send_sem=send_sem.at[i], recv_sem=recv_sem.at[i],
            device_id=(r + dr, c + dc), device_id_type=MESH,
        )

    def put(name, src=None, only=None):
        copy = message(name, send.at[SLOT[name]] if src is None else src)
        there = has[MESSAGES[name]]

        @pl.when(there if only is None else there & (c % 2 == only))
        def _():
            copy.start()

        started[name] = there, copy

    def flush(name, only):
        there, copy = started[name]
        flushed[name] = only

        @pl.when(there & (c % 2 == only))
        def _():
            copy.wait_send()

    def got(name):
        dr, dc = MESSAGES[name]
        with jax.named_scope("wait_" + name):
            @pl.when(has[-dr, -dc])
            def _():
                message(name, recv.at[SLOT[name]]).wait_recv()

        return recv[SLOT[name]]

    def fill(name, value):
        if name not in filled:
            filled.add(name)
            send[SLOT[name]] = value()

    place_copy = pltpu.make_async_remote_copy(
        src_ref=place, dst_ref=place_in, send_sem=place_send, recv_sem=place_recv,
        device_id=(r + 1, c), device_id_type=MESH,
    )
    with jax.named_scope("wait_load"):
        loads[1].wait()

    first = {
        "t": ("obj_ht", obj.at[:, TOP, LEFT]),
        "b": ("obj_hb", obj.at[:, BOTTOM, LEFT]),
        "r": ("obj_vr", obj.at[:, TOP, RIGHT]),
    }
    for k, only in order(CFG["R1pre"]):
        put(*first[k], only)

    loads[0].wait()
    dy = pos[0]
    dx = pos[1]
    rows = lax.broadcasted_iota(jnp.int32, (W, W), 0)
    cols = lax.broadcasted_iota(jnp.int32, (W, W), 1)
    below = rows < dy
    beside = cols < dx
    place[...] = jnp.full((8, W), dx.astype(F32))

    @pl.when(has[DOWN])
    def _():
        place_copy.start()

    def build_tables():
        re_high, re_low, im_high, im_low = (table[i] for i in range(4))
        blocks = [
            (re_high, im_high), (re_high, im_high), (re_low, im_low),
            (-im_high, re_high), (-im_high, re_high), (-im_low, re_low),
        ]
        for b, (real, imag) in enumerate(blocks):
            span = pl.ds(b * N, N)
            right_table[span, pl.ds(0, N)] = real
            right_table[span, pl.ds(N, N)] = imag
            for half in range(2):
                left_table[pl.ds(half * N, W), span] = real[half * W : (half + 1) * W]
                left_table[pl.ds(half * N + W, W), span] = imag[half * W : (half + 1) * W]

    def turn_probe():
        for part in range(2):
            turned = pltpu.roll(probe[part], dy, 0)
            probe[part] = pltpu.roll(turned, dx, 1)

    loads[2].wait()
    build_tables()

    @pl.when(has[UP])
    def _():
        place_copy.wait_recv()

    beside_above = cols.astype(F32) < place_in[0:1, :]

    for name in CFG["R1x"]:
        flush(name, 0)

    fill("obj_vl", lambda: jnp.where(beside_above, got("obj_ht"), obj[:, TOP, LEFT]))
    put("obj_vl")
    for k, only in order(CFG["R1post"]):
        put(*first[k], only)
    loads[3].wait()
    turn_probe()

    def put_stack(span_rows, span_cols, real, imag):
        for base, value in ((0, real), (3, imag)):
            high, low = split(value)
            for b, item in ((0, high), (1, low), (2, high)):
                stack[span_rows, pl.ds((base + b) * N + span_cols, item.shape[1])] = item

    def put_stack2(row, real, imag):
        for base, value in ((0, real), (3, imag)):
            high, low = split(value)
            for b, item in ((0, high), (1, low), (2, high)):
                stack2[pl.ds((base + b) * N + row, item.shape[0]), :] = item

    def exit_wave(half, quarter_left, quarter_right):
        span = TOP if half == 0 else BOTTOM
        for side, patch in ((0, quarter_left), (1, quarter_right)):
            lanes = pl.ds(side * W, W)
            pr, pi = probe[0, span, lanes], probe[1, span, lanes]
            put_stack(
                span, side * W,
                pr * patch[0] - pi * patch[1], pr * patch[1] + pi * patch[0],
            )

    def right_product(half):
        span = pl.ds(half * W, W)
        out = jnp.dot(stack[span, :], right_table[...], preferred_element_type=F32)
        put_stack2(half * W, out[:, :N], out[:, N:])

    def left_product(half):
        out = jnp.dot(
            left_table[pl.ds(half * N, N), :], stack2[...], preferred_element_type=F32
        )
        return out[:W], out[W:]

    def back_product(half):
        span = pl.ds(half * W, W)
        back_re, back_im = left_product(half)
        pr, pi = probe[0, span, :], probe[1, span, :]
        grad[0, span, :] = pr * back_re - pi * back_im
        grad[1, span, :] = -(pr * back_im) - pi * back_re

    def sweep(source, low_left, low_right, right_top, right_bottom):
        for k in CFG["sweep"]:
            if k == "t":
                top_right = jnp.where(below, low_right(), source[:, TOP, RIGHT])
                own = jnp.where(beside, right_top(), source[:, TOP, LEFT])
                exit_wave(0, jnp.where(below, low_left(), own), top_right)
                right_product(0)
            else:
                bottom = jnp.where(beside, right_bottom(), source[:, BOTTOM, LEFT])
                exit_wave(1, bottom, source[:, BOTTOM, RIGHT])
                right_product(1)
        for half in range(2):
            far_re, far_im = left_product(half)
            misfit = far_re * far_re + far_im * far_im - meas[pl.ds(half * W, W), :]
            put_stack(pl.ds(half * W, W), 0, misfit * far_re, -(misfit * far_im))
        for part in range(2):
            out = jnp.dot(
                stack[...], right_table[:, pl.ds(part * N, N)], preferred_element_type=F32
            )
            high, low = split(out)
            for b, item in ((0, high), (1, low), (2, high)):
                stack2[pl.ds((3 * part + b) * N, N), :] = item

    def update(old_obj, old_vel, new_obj, new_vel, span_r, span_c, gradient):
        speed = MOMENTUM * old_vel[:, span_r, span_c] + gradient
        moved = old_obj[:, span_r, span_c] - STEP * speed
        new_vel[:, span_r, span_c] = speed
        new_obj[:, span_r, span_c] = moved
        return moved

    loads[4].wait()
    sweep(
        obj, lambda: got("obj_vl"), lambda: got("obj_vr"),
        lambda: recv[SLOT["obj_ht"]], lambda: got("obj_hb"),
    )
    back_product(0)
    fill("grad_vl", lambda: jnp.where(below, grad[:, TOP, LEFT], 0.0))
    put("grad_vl")
    loads[5].wait()

    def coasting(span_r, span_c):
        return obj[:, span_r, span_c] - (STEP * MOMENTUM) * vel[:, span_r, span_c]

    def send_r(only):
        fill("grad_vr", lambda: jnp.where(below, grad[:, TOP, RIGHT], 0.0))
        put("grad_vr", only=only)

    def send_R(only):
        fill("next_vr", lambda: coasting(TOP, RIGHT) - STEP * jnp.where(below, 0.0, grad[:, TOP, RIGHT]))
        put("next_vr", only=only)

    def send_b(only):
        fill("grad_hb", lambda: jnp.where(beside, grad[:, BOTTOM, LEFT], 0.0))
        put("grad_hb", only=only)

    def send_B(only):
        fill("next_hb", lambda: coasting(BOTTOM, LEFT) - STEP * jnp.where(beside, 0.0, grad[:, BOTTOM, LEFT]))
        put("next_hb", only=only)

    sends = {"r": send_r, "R": send_R, "b": send_b, "B": send_B}
    for k, only in order(CFG["mid"]):
        if k == "|":
            back_product(1)
        else:
            sends[k](only)

    above = got("grad_vl")
    across = jnp.where(beside & ~below, grad[:, TOP, LEFT], 0.0) + jnp.where(beside_above, above, 0.0)
    kept = jnp.where(below | beside, 0.0, grad[:, TOP, LEFT]) + jnp.where(beside_above, 0.0, above)
    halo[0] = across
    halo[1] = kept

    def send_h(only):
        fill("grad_ht", lambda: halo[0])
        put("grad_ht", only=only)

    def send_H(only):
        fill("next_ht", lambda: coasting(TOP, LEFT) - STEP * halo[1])
        put("next_ht", only=only)

    sends |= {
        "h": send_h, "H": send_H,
        "w": lambda only: flush("grad_ht", only), "W": lambda only: flush("next_ht", only),
    }
    for k, only in order(CFG["mid2"]):
        sends[k](only)

    step_right = jnp.where(has[TO_RIGHT], STEP, 0.0)
    step_down = jnp.where(has[DOWN], STEP, 0.0)
    moving = (obj, vel, obj1, vel1)
    update(*moving, BOTTOM, RIGHT, grad[:, BOTTOM, RIGHT])
    moved = update(*moving, TOP, LEFT, halo[1] + got("grad_ht"))
    right_top = got("next_ht") - step_right * halo[0]
    halo[0] = right_top
    fill("next_vl", lambda: jnp.where(beside_above, right_top, moved))
    put("next_vl")
    update(*moving, BOTTOM, LEFT, jnp.where(beside, 0.0, grad[:, BOTTOM, LEFT]) + got("grad_hb"))

    def low_right():
        update(*moving, TOP, RIGHT, jnp.where(below, 0.0, grad[:, TOP, RIGHT]) + got("grad_vr"))
        return got("next_vr") - step_down * jnp.where(below, grad[:, TOP, RIGHT], 0.0)

    def right_bottom():
        return got("next_hb") - step_right * jnp.where(beside, grad[:, BOTTOM, LEFT], 0.0)

    sweep(obj1, lambda: got("next_vl"), low_right, lambda: halo[0], right_bottom)
    back_product(0)
    fill("last_vl", lambda: jnp.where(below, grad[:, TOP, LEFT], 0.0))
    put("last_vl")

    def last_r(only):
        fill("last_vr", lambda: jnp.where(below, grad[:, TOP, RIGHT], 0.0))
        put("last_vr", only=only)

    def last_b(only):
        fill("last_hb", lambda: jnp.where(beside, grad[:, BOTTOM, LEFT], 0.0))
        put("last_hb", only=only)

    lasts = {"r": last_r, "b": last_b, "|": lambda only: back_product(1)}
    for k, only in order(CFG["R4pre"]):
        lasts[k](only)
    above = got("last_vl")
    fill("last_ht", lambda: jnp.where(beside & ~below, grad[:, TOP, LEFT], 0.0) + jnp.where(beside_above, above, 0.0))
    put("last_ht")
    for k, only in order(CFG["R4post"]):
        lasts[k](only)

    moving = (obj1, vel1, obj_out, vel_out)

    def finish(span_r, span_c, gradient):
        update(*moving, span_r, span_c, gradient)

    finish(BOTTOM, RIGHT, grad[:, BOTTOM, RIGHT])
    finish(TOP, RIGHT, jnp.where(below, 0.0, grad[:, TOP, RIGHT]) + got("last_vr"))
    kept = jnp.where(below | beside, 0.0, grad[:, TOP, LEFT]) + jnp.where(beside_above, 0.0, recv[SLOT["last_vl"]])
    if CFG["R4post"]:
        finish(TOP, LEFT, kept + got("last_ht"))
        finish(BOTTOM, LEFT, jnp.where(beside, 0.0, grad[:, BOTTOM, LEFT]) + got("last_hb"))
    else:
        finish(BOTTOM, LEFT, jnp.where(beside, 0.0, grad[:, BOTTOM, LEFT]) + got("last_hb"))
        finish(TOP, LEFT, kept + got("last_ht"))

    for name, (there, copy) in started.items():
        @pl.when(there & (c % 2 != flushed[name]) if name in flushed else there)
        def _():
            copy.wait_send()

    @pl.when(has[DOWN])
    def _():
        place_copy.wait_send()


def write_kernel(obj, vel, obj_out, vel_out, sem):
    copies = [
        pltpu.make_async_copy(src.at[part], dst.at[part], sem.at[2 * i + part])
        for i, (src, dst) in enumerate([(obj, obj_out), (vel, vel_out)])
        for part in range(2)
    ]
    for copy in copies:
        copy.start()
    for copy in copies:
        copy.wait()


def on_device(n_rows, n_cols, object_field, velocity, positions, measured, probe):
    vmem = lambda *shape: pltpu.VMEM(shape, F32)
    anywhere = pl.BlockSpec(memory_space=pl.ANY)
    count = len(MESSAGES)
    results = pl.pallas_call(
        functools.partial(kernel, n_rows, n_cols),
        out_shape=(pltpu.VMEM((2, N, N), F32), pltpu.VMEM((2, N, N), F32)),
        in_specs=[anywhere] * 6,
        out_specs=(pl.BlockSpec(memory_space=pltpu.VMEM),) * 2,
        scratch_shapes=[
            pltpu.SMEM((2,), jnp.int32),
            vmem(2, N, N), vmem(2, N, N), vmem(2, N, N), vmem(2, N, N),
            vmem(N, N), vmem(2, N, N),
            pltpu.VMEM((4, N, N), BF16),
            pltpu.VMEM((6 * N, 2 * N), BF16),
            pltpu.VMEM((2 * N, 6 * N), BF16),
            pltpu.VMEM((N, 6 * N), BF16),
            pltpu.VMEM((6 * N, N), BF16),
            vmem(2, N, N), vmem(2, 2, W, W),
            vmem(count, 2, W, W), vmem(count, 2, W, W),
            vmem(8, W), vmem(8, W),
            pltpu.SemaphoreType.DMA((6,)),
            pltpu.SemaphoreType.DMA((count,)), pltpu.SemaphoreType.DMA((count,)),
            pltpu.SemaphoreType.DMA, pltpu.SemaphoreType.DMA,
        ],
        compiler_params=pltpu.CompilerParams(collective_id=0, has_side_effects=True),
        name="ptycho",
    )(
        positions.reshape(2), object_field, velocity, measured.reshape(N, N), probe,
        jnp.asarray(fourier_tables()),
    )
    field = jax.ShapeDtypeStruct((2, N, N), F32)
    return pl.pallas_call(
        write_kernel,
        out_shape=(field, field),
        in_specs=[pl.BlockSpec(memory_space=pltpu.VMEM)] * 2,
        out_specs=(anywhere, anywhere),
        scratch_shapes=[pltpu.SemaphoreType.DMA((4,))],
        name="write",
    )(*(pltpu.with_memory_space_constraint(x, pltpu.VMEM) for x in results))


def solution(mesh):
    placed = (
        P(None, "row", "col"),
        P(None, "row", "col"),
        P("row", "col", None, None),
        P("row", "col", None, None, None),
        P(),
    )
    return jax.shard_map(
        functools.partial(on_device, mesh.shape["row"], mesh.shape["col"]),
        mesh=mesh,
        in_specs=placed,
        out_specs=(P(None, "row", "col"), P(None, "row", "col")),
        check_vma=False,
    )
```
